32 devices in a mesh: node: 8 (over y, x, core), grp: 4 (over z).
Axes of the slice: x: 2, y: 2, z: 4, core: 2. Of those that a mesh axis runs over, the one named last changes fastest.
Arguments:
- tokens: bfloat16 [12288, 1792], P(('node', 'grp')), may hold values from -6 to 6
- cotangent: bfloat16 [12288, 1792], P(('node', 'grp')), may hold values from -6 to 6
- gate_weight: bfloat16 [1792, 1024], P('node'), may hold values from -0.125 to 0.125
- up_weight: bfloat16 [1792, 1024], P('node'), may hold values from -0.125 to 0.125
- down_weight_t: bfloat16 [1792, 1024], P('node'), may hold values from -0.125 to 0.125
- error_memory: bfloat16 [4, 1792, 3072], P('grp', 'node'), may hold values from -4 to 4
- q_init: float32 [3, 1024, 32], replicated, may hold values from -6 to 6
Outputs:
- token_grad: bfloat16 [12288, 1792], P(('node', 'grp'))
- new_error: bfloat16 [4, 1792, 3072], P('grp', 'node')
- p_hat: float32 [3, 1792, 32], P(None, 'node')
- q_new: float32 [3, 1024, 32], replicated
The draws below stay inside these ranges and needn't reach their ends.
All inputs are finite; a program needn't handle non-finite values.
Results may differ from the reference program's by a relative error of at most 0.012.
Values may be sent and summed in bfloat16 or wider, within the bound.
A program may use at most 192 MiB of HBM per device.

```python
import math
import jax
import jax.numpy as jnp
from jax import lax

D = 1792
H = 1024
R = 32
TOK_DEV = 384
TOKENS = 12288
N_NODE = 8
N_GRP = 4


def block_levels(rng, dims, cuts, least, high):
    factor_of, own = 1.0, jax.random.fold_in(rng, 6)
    for position, parts in cuts:
        heights = jnp.exp(jax.random.uniform(jax.random.fold_in(own, position), (parts,), jnp.float32, least / len(cuts), high / len(cuts)))
        factor_of = factor_of * jnp.repeat(heights, dims[position] // parts).reshape([-1 if axis == position else 1 for axis in range(len(dims))])
    return factor_of


def normal_values(own_key, extent, scale, bound, pieces=(), kind=jnp.bfloat16):
    entries = jax.random.normal(own_key, extent, jnp.float32) * scale
    if len(pieces) > 0:
        entries = block_levels(own_key, extent, pieces, -0.22, 0.18) * entries
    return jnp.clip(entries, min=-bound, max=bound).astype(kind)


def setup_inputs(seed: int = 0) -> dict:
    arg_keys = jax.random.split(jax.random.key(seed), 8)
    return {
        "tokens": normal_values(arg_keys[0], (TOKENS, D), 1.0, 6.0, ((0, 32),)),
        "cotangent": normal_values(arg_keys[1], (TOKENS, D), 1.0, 6.0, ((0, 32),)),
        "gate_weight": normal_values(arg_keys[2], (D, H), D ** -0.5, 0.125, ((0, 8),)),
        "up_weight": normal_values(arg_keys[3], (D, H), D ** -0.5, 0.125, ((0, 8),)),
        "down_weight_t": normal_values(arg_keys[4], (D, H), D ** -0.5, 0.125, ((0, 8),)),
        "error_memory": normal_values(arg_keys[5], (N_GRP, D, 3 * H), 0.5, 4.0, ((0, 4), (1, 8))),
        "q_init": normal_values(arg_keys[6], (3, H, R), 1.0, 6.0, (), jnp.float32),
    }


def gelu_parts(value):
    coeff = math.sqrt(2.0 / math.pi)
    inner = coeff * (value + 0.044715 * value * value * value)
    tanh_value = jnp.tanh(inner)
    activation = 0.5 * value * (1.0 + tanh_value)
    slope = 0.5 * (1.0 + tanh_value) + 0.5 * value * (1.0 - tanh_value * tanh_value) * coeff * (1.0 + 3.0 * 0.044715 * value * value)
    return (activation, slope)

def arrange(values):
    return values.reshape(N_NODE, N_GRP, TOK_DEV, -1).transpose(1, 0, 2, 3).reshape(N_GRP, N_NODE * TOK_DEV, -1)

def group_grad(items):
    token_rows, cot_rows, gate_up, hidden = items
    left_part = jnp.dot(token_rows.T.astype(jnp.float32), gate_up.astype(jnp.float32), preferred_element_type=jnp.float32)
    right_part = jnp.dot(cot_rows.T.astype(jnp.float32), hidden.astype(jnp.float32), preferred_element_type=jnp.float32)
    return jnp.concatenate([left_part, right_part], axis=1)

def reference(tokens, cotangent, gate_weight, up_weight, down_weight_t, error_memory, q_init):
    hidden_units = gate_weight.shape[1]
    gate_pre = jnp.dot(tokens.astype(jnp.float32), gate_weight.astype(jnp.float32), preferred_element_type=jnp.float32)
    up_pre = jnp.dot(tokens.astype(jnp.float32), up_weight.astype(jnp.float32), preferred_element_type=jnp.float32)
    activation, slope = gelu_parts(gate_pre)
    hidden = (activation * up_pre).astype(jnp.bfloat16)
    back_hidden = jnp.dot(cotangent.astype(jnp.float32), down_weight_t.astype(jnp.float32), preferred_element_type=jnp.float32)
    grad_up = (back_hidden * activation).astype(jnp.bfloat16)
    grad_gate = (back_hidden * up_pre * slope).astype(jnp.bfloat16)
    token_grad = (jnp.dot(grad_gate.astype(jnp.float32), gate_weight.T.astype(jnp.float32), preferred_element_type=jnp.float32) + jnp.dot(grad_up.astype(jnp.float32), up_weight.T.astype(jnp.float32), preferred_element_type=jnp.float32)).astype(jnp.bfloat16)
    gate_up = jnp.concatenate([grad_gate, grad_up], axis=1)
    grads = lax.map(group_grad, (arrange(tokens), arrange(cotangent), arrange(gate_up), arrange(hidden)))
    grad_scale = 1.0 / math.sqrt(TOK_DEV * N_NODE)
    merged = grads * grad_scale + error_memory.astype(jnp.float32)
    hats = []
    rights = []
    errors = []
    for m in range(3):
        matrix_block = merged[:, :, m * hidden_units:(m + 1) * hidden_units]
        power = jnp.einsum('kdh,hr->dr', matrix_block, q_init[m], precision=lax.Precision.HIGHEST) / N_GRP
        gram_matrix = jnp.dot(power.T, power, precision=lax.Precision.HIGHEST)
        factor = jnp.linalg.cholesky(gram_matrix)
        left_hat = jax.scipy.linalg.solve_triangular(factor, power.T, lower=True).T
        right_new = jnp.einsum('kdh,dr->hr', matrix_block, left_hat, precision=lax.Precision.HIGHEST) / N_GRP
        rebuilt = jnp.dot(left_hat, right_new.T, precision=lax.Precision.HIGHEST)
        errors.append(matrix_block - rebuilt[None])
        hats.append(left_hat)
        rights.append(right_new)
    new_error = jnp.concatenate(errors, axis=2).astype(jnp.bfloat16)
    return (token_grad, new_error, jnp.stack(hats), jnp.stack(rights))
```

```python
import functools
import math

import jax
import jax.numpy as jnp
from jax import lax
from jax.experimental import pallas as pl
from jax.experimental.pallas import tpu as pltpu
from jax.sharding import PartitionSpec as P

MESH = pl.DeviceIdType.MESH
F32, BF16 = jnp.float32, jnp.bfloat16
HIGHEST = lax.Precision.HIGHEST
LANES = 128


def gelu_parts(value):
    coeff = math.sqrt(2.0 / math.pi)
    square = value * value
    tanh_value = jnp.tanh(coeff * (value + 0.044715 * square * value))
    activation = 0.5 * value * (1.0 + tanh_value)
    slope = 0.5 * (1.0 + tanh_value) + 0.5 * value * (1.0 - tanh_value * tanh_value) * coeff * (
        1.0 + 3.0 * 0.044715 * square
    )
    return activation, slope


def dot(a, b, precision=None):
    return jnp.dot(a, b, preferred_element_type=F32, precision=precision)


def dot_nt(a, b, precision=None):
    return lax.dot_general(
        a, b, (((1,), (1,)), ((), ())), preferred_element_type=F32, precision=precision
    )


def subsets(items):
    found = [()]
    for item in items:
        found += [s + (item,) for s in found]
    return found


def kernel(
    n, g, rank, n_recv,
    tok, cot, w_gate, w_up, w_down, err, q_pad,
    tok_grad, new_err, p_out, q_out,
    full, tok_t, cot_t, act, ups, hid, d_up, d_gate, grads, *rest
):
    recv_bufs = rest[:n_recv]
    (merged, power, hat, block_diag, q_t, pw_all, gram_all, q_part, q_rs, q_grp, q_all,
     send_sems, recv_sems, local_sems) = rest[n_recv:]
    me, grp = lax.axis_index("node"), lax.axis_index("grp")
    rows, hidden = w_gate.shape
    depth = tok.shape[1]
    half = hidden // 2
    bits = n.bit_length() - 1
    tile = 256
    used = 3 * rank
    weights = (w_gate, w_up, w_down)

    barrier = pltpu.get_barrier_semaphore()
    for d in range(1, n):
        pl.semaphore_signal(barrier, inc=1, device_id=(lax.rem(me + d, n), grp), device_id_type=MESH)
    for d in range(1, g):
        pl.semaphore_signal(barrier, inc=1, device_id=(me, lax.rem(grp + d, g)), device_id_type=MESH)

    flip = [(1 << b) * (1 - 2 * lax.rem(me // (1 << b), 2)) for b in range(bits)]
    offset = lambda mask: sum((flip[b] for b in mask), 0)
    outer = list(range(1, bits))
    orders = [outer + [0], outer[::-1] + [0]]
    rs_orders = [[0] + outer, [0] + outer[::-1]]
    cols = [pl.ds(h * half, half) for h in range(2)]
    block = lambda index: pl.ds(pl.multiple_of(index * rows, rows), rows)

    count = [0]
    started = []

    def send(src, dst, node, group):
        copy = pltpu.make_async_remote_copy(
            src_ref=src, dst_ref=dst,
            send_sem=send_sems.at[count[0]], recv_sem=recv_sems.at[count[0]],
            device_id=(node, group), device_id_type=MESH,
        )
        count[0] += 1
        started.append(copy)
        copy.start()
        return copy

    locals_ = []
    for w in range(3):
        copy = pltpu.make_async_copy(weights[w], full.at[w, block(me)], local_sems.at[w])
        copy.start()
        locals_.append(copy)
    pl.semaphore_wait(barrier, n - 1 + g - 1)

    gathers = {}

    def gather_start(w, t):
        for h in range(2):
            bit = orders[h][t]
            gathers[w, t, h] = []
            for mask in subsets(orders[h][:t]):
                at = (w, block(me + offset(mask)), cols[h])
                src = weights[w].at[:, cols[h]] if t == 0 else full.at[at]
                gathers[w, t, h].append(send(src, full.at[at], me + flip[bit], grp))

    def gather_finish(w, t):
        for h in range(2):
            for copy in gathers[w, t, h]:
                copy.wait_recv()

    for w in range(3):
        gather_start(w, 0)

    @pl.loop(0, depth // tile)
    def _(i):
        at = pl.ds(pl.multiple_of(i * tile, tile), tile)
        tok_t[at, :] = tok[:, at].T
        cot_t[at, :] = cot[:, at].T

    merged[...] = jnp.zeros_like(merged)
    power[...] = jnp.zeros_like(power)
    hat[...] = jnp.zeros_like(hat)
    block_diag[...] = jnp.zeros_like(block_diag)
    q_t[...] = jnp.zeros_like(q_t)
    for copy in locals_:
        copy.wait()

    for t in range(1, bits - 1):
        for w in range(3):
            gather_finish(w, t - 1)
            gather_start(w, t)
    for w in range(2):
        gather_finish(w, bits - 2)
        gather_start(w, bits - 1)

    gather_finish(0, bits - 1)

    @pl.loop(0, hidden // tile)
    def _(j):
        at = pl.ds(pl.multiple_of(j * tile, tile), tile)
        act[:, at] = dot(tok[...], full[0, :, at])

    gather_finish(1, bits - 1)

    @pl.loop(0, hidden // tile)
    def _(j):
        at = pl.ds(pl.multiple_of(j * tile, tile), tile)
        up_pre = dot(tok[...], full[1, :, at])
        activation, slope = gelu_parts(act[:, at])
        act[:, at] = activation
        ups[:, at] = up_pre * slope
        hid[:, at] = (activation * up_pre).astype(BF16)

    reduces = {}

    def partial_grad(m, left, right):
        @pl.loop(0, depth // tile)
        def _(i):
            at = pl.ds(pl.multiple_of(i * tile, tile), tile)
            grads[m, at, :] = dot(left[at, :], right[...]).astype(BF16)

    def reduce_start(m, t):
        for h in range(2):
            bit = rs_orders[h][t]
            reduces[m, t, h] = []
            for slot, mask in enumerate(subsets(rs_orders[h][t + 1:])):
                src = grads.at[m, block(me + flip[bit] + offset(mask)), cols[h]]
                dst = recv_bufs[t].at[m, slot, :, cols[h]]
                reduces[m, t, h].append(send(src, dst, me + flip[bit], grp))

    def reduce_add(m, t):
        for h in range(2):
            for slot, mask in enumerate(subsets(rs_orders[h][t + 1:])):
                reduces[m, t, h][slot].wait_recv()
                at = block(me + offset(mask))
                total = (
                    grads[m, at, cols[h]].astype(F32) + recv_bufs[t][m, slot, :, cols[h]].astype(F32)
                )
                if t < bits - 1:
                    grads[m, at, cols[h]] = total.astype(BF16)
                else:
                    scale = 1.0 / math.sqrt(tok.shape[0] * n)
                    memory = err[0, :, pl.ds(m * hidden + h * half, half)].astype(F32)
                    merged[m, 0:rows, cols[h]] = total * scale + memory

    def advance(m, t):
        reduce_add(m, t - 1)
        reduce_start(m, t)

    partial_grad(2, cot_t, hid)
    reduce_start(2, 0)
    gather_finish(2, bits - 2)
    gather_start(2, bits - 1)
    gather_finish(2, bits - 1)

    @pl.loop(0, hidden // tile)
    def _(j):
        at = pl.ds(pl.multiple_of(j * tile, tile), tile)
        back = dot(cot[...], full[2, :, at])
        d_up[:, at] = (back * act[:, at]).astype(BF16)
        d_gate[:, at] = (back * ups[:, at]).astype(BF16)

    advance(2, 1)
    partial_grad(0, tok_t, d_gate)
    reduce_start(0, 0)
    partial_grad(1, tok_t, d_up)
    reduce_start(1, 0)
    advance(0, 1)

    def token_part(first, last):
        @pl.loop(first, last)
        def _(i):
            at = pl.ds(pl.multiple_of(i * tile, tile), tile)
            tok_grad[:, at] = (
                dot_nt(d_gate[...], full[0, at, :]) + dot_nt(d_up[...], full[1, at, :])
            ).astype(BF16)

    steps = depth // tile
    token_part(0, steps // 2)
    advance(1, 1)
    advance(2, 2)
    token_part(steps // 2, steps)
    advance(0, 2)
    advance(1, 2)
    for t in range(3, bits):
        for m in (2, 0, 1):
            advance(m, t)
    total = jnp.zeros((rows, LANES), F32)
    for m in (2, 0, 1):
        reduce_add(m, bits - 1)
        total += dot(merged[m, 0:rows, :], q_pad[m], HIGHEST)

    pw_all[grp] = total.astype(BF16)
    copies = [
        send(pw_all.at[grp], pw_all.at[grp], me, lax.rem(grp + d, g)) for d in range(1, g)
    ]
    for copy in copies:
        copy.wait_recv()
    total = pw_all[0].astype(F32)
    for k in range(1, g):
        total += pw_all[k].astype(F32)
    power[0:rows, :] = total * (1.0 / g)

    lane = lax.broadcasted_iota(jnp.int32, (rank, LANES), 1)
    row = lax.broadcasted_iota(jnp.int32, (rank, LANES), 0)
    padded = power[...]
    gram = dot(padded.T, padded, HIGHEST)
    picked = gram[0:rank]
    for m in range(1, 3):
        picked = jnp.where(lane >= m * rank, gram[m * rank:(m + 1) * rank], picked)
    gram_all[me] = picked
    copies = [
        send(gram_all.at[me], gram_all.at[me], lax.rem(me + d, n), grp) for d in range(1, n)
    ]
    for copy in copies:
        copy.wait_recv()
    picked = gram_all[0]
    for k in range(1, n):
        picked += gram_all[k]

    work = []
    for m in range(3):
        rolled = picked if m == 0 else pltpu.roll(picked, LANES - m * rank, 1)
        unit = jnp.where(lane == row + rank, 1.0, 0.0).astype(F32)
        work.append(jnp.where(lane < rank, rolled, unit))
    for j in range(rank):
        for m in range(3):
            a = work[m]
            inverse = 1.0 / jnp.sqrt(a[j:j + 1, j:j + 1])
            pivot_row = a[j:j + 1, :] * inverse
            column = a[:, j:j + 1] * inverse
            work[m] = jnp.where(row > j, a - column * pivot_row, jnp.where(row == j, pivot_row, a))
    for m in range(3):
        shift = ((m - 1) * rank) % LANES
        moved = work[m] if shift == 0 else pltpu.roll(work[m], shift, 1)
        inside = (lane >= m * rank) & (lane < (m + 1) * rank)
        block_diag[m * rank:(m + 1) * rank, :] = jnp.where(inside, moved, 0.0)
    hat[0:rows, :] = dot_nt(power[0:rows, :], block_diag[...], HIGHEST)
    p_out[...] = hat[0:rows, :]

    hat_t = hat[...].T
    c_blocks = min(n, hidden // LANES)
    r_blocks = n // c_blocks
    c_size, r_size = hidden // c_blocks, used // r_blocks
    for m in range(3):
        q_t[m * rank:(m + 1) * rank, :] = dot(hat_t[m * rank:(m + 1) * rank], merged[m], HIGHEST)
    spots = [
        (slice(c // c_blocks * r_size, (c // c_blocks + 1) * r_size),
         slice(c % c_blocks * c_size, (c % c_blocks + 1) * c_size))
        for c in range(n)
    ]
    for c in range(n):
        q_part[c] = q_t[spots[c]].astype(BF16)
    q_rs[me] = q_part[me]
    copies = []
    for d in range(1, n):
        to = lax.rem(me + d, n)
        copies.append(send(q_part.at[to], q_rs.at[me], to, grp))
    for copy in copies:
        copy.wait_recv()
    total = q_rs[0].astype(F32)
    for k in range(1, n):
        total += q_rs[k].astype(F32)
    q_grp[grp] = total.astype(BF16)
    copies = [send(q_grp.at[grp], q_grp.at[grp], me, lax.rem(grp + d, g)) for d in range(1, g)]
    for copy in copies:
        copy.wait_recv()
    total = q_grp[0].astype(F32)
    for k in range(1, g):
        total += q_grp[k].astype(F32)
    q_all[me] = (total * (1.0 / g)).astype(BF16)
    copies = [send(q_all.at[me], q_all.at[me], lax.rem(me + d, n), grp) for d in range(1, n)]
    for copy in copies:
        copy.wait_recv()
    for c in range(n):
        q_t[spots[c]] = q_all[c].astype(F32)
    q_out[...] = q_t[0:used, :]

    wide = lax.broadcasted_iota(jnp.int32, (rows, LANES), 1)
    for m in range(3):
        own = jnp.where((wide >= m * rank) & (wide < (m + 1) * rank), hat[0:rows, :], 0.0)
        for h in range(2):
            rebuilt = dot(own, q_t[:, cols[h]], HIGHEST)
            new_err[0, :, pl.ds(m * hidden + h * half, half)] = (
                merged[m, 0:rows, cols[h]] - rebuilt
            ).astype(BF16)
    for copy in started:
        copy.wait_send()


def on_device(n, g, tokens, cotangent, gate_weight, up_weight, down_weight_t, error_memory, q_init):
    token_rows, depth = tokens.shape
    rows, hidden = gate_weight.shape
    rank = q_init.shape[2]
    used = 3 * rank
    bits = n.bit_length() - 1
    padded = -(-rows // LANES) * LANES
    q_pad = jnp.stack(
        [jnp.pad(q_init[m], ((0, 0), (m * rank, LANES - (m + 1) * rank))) for m in range(3)]
    )
    c_blocks = min(n, hidden // LANES)
    chunk = (used // (n // c_blocks), hidden // c_blocks)
    copies = 12 * (n - 1) + 3 * (n - 1) + 2 * (g - 1)
    recv_shapes = [
        pltpu.VMEM((3, 1 << (bits - 1 - t), rows, hidden), BF16) for t in range(bits)
    ]
    vmem = pl.BlockSpec(memory_space=pltpu.VMEM)
    token_grad, new_error, hats, q_t = pl.pallas_call(
        functools.partial(kernel, n, g, rank, bits),
        out_shape=(
            jax.ShapeDtypeStruct((token_rows, depth), BF16),
            jax.ShapeDtypeStruct((1, rows, 3 * hidden), BF16),
            jax.ShapeDtypeStruct((rows, LANES), F32),
            jax.ShapeDtypeStruct((used, hidden), F32),
        ),
        in_specs=[vmem] * 7,
        out_specs=(vmem,) * 4,
        scratch_shapes=[
            pltpu.VMEM((3, depth, hidden), BF16),
            pltpu.VMEM((depth, token_rows), BF16),
            pltpu.VMEM((depth, token_rows), BF16),
            pltpu.VMEM((token_rows, hidden), F32),
            pltpu.VMEM((token_rows, hidden), F32),
            pltpu.VMEM((token_rows, hidden), BF16),
            pltpu.VMEM((token_rows, hidden), BF16),
            pltpu.VMEM((token_rows, hidden), BF16),
            pltpu.VMEM((3, depth, hidden), BF16),
            *recv_shapes,
            pltpu.VMEM((3, padded, hidden), F32),
            pltpu.VMEM((padded, LANES), F32),
            pltpu.VMEM((padded, LANES), F32),
            pltpu.VMEM((LANES, LANES), F32),
            pltpu.VMEM((LANES, hidden), F32),
            pltpu.VMEM((g, rows, LANES), BF16),
            pltpu.VMEM((n, rank, LANES), F32),
            pltpu.VMEM((n,) + chunk, BF16),
            pltpu.VMEM((n,) + chunk, BF16),
            pltpu.VMEM((g,) + chunk, BF16),
            pltpu.VMEM((n,) + chunk, BF16),
            pltpu.SemaphoreType.DMA((copies,)),
            pltpu.SemaphoreType.DMA((copies,)),
            pltpu.SemaphoreType.DMA((3,)),
        ],
        compiler_params=pltpu.CompilerParams(
            collective_id=0, has_side_effects=True, vmem_limit_bytes=67_043_328
        ),
    )(tokens, cotangent, gate_weight, up_weight, down_weight_t, error_memory, q_pad)
    p_hat = jnp.stack([hats[:, m * rank:(m + 1) * rank] for m in range(3)])
    q_new = q_t.reshape(3, rank, hidden).transpose(0, 2, 1)
    return token_grad, new_error, p_hat, q_new


def solution(mesh):
    return jax.shard_map(
        functools.partial(on_device, mesh.shape["node"], mesh.shape["grp"]),
        mesh=mesh,
        in_specs=(
            P(("node", "grp"), None),
            P(("node", "grp"), None),
            P("node", None),
            P("node", None),
            P("node", None),
            P("grp", "node", None),
            P(),
        ),
        out_specs=(P(("node", "grp"), None), P("grp", "node", None), P(None, "node", None), P()),
        check_vma=False,
    )
```

```python
import functools
import math

import jax
import jax.numpy as jnp
from jax import lax
from jax.experimental import pallas as pl
from jax.experimental.pallas import tpu as pltpu
from jax.sharding import PartitionSpec as P

MESH = pl.DeviceIdType.MESH
F32, BF16 = jnp.float32, jnp.bfloat16
HIGHEST = lax.Precision.HIGHEST
LANES = 128


def gelu_parts(value):
    coeff = math.sqrt(2.0 / math.pi)
    square = value * value
    tanh_value = jnp.tanh(coeff * (value + 0.044715 * square * value))
    activation = 0.5 * value * (1.0 + tanh_value)
    slope = 0.5 * (1.0 + tanh_value) + 0.5 * value * (1.0 - tanh_value * tanh_value) * coeff * (
        1.0 + 3.0 * 0.044715 * square
    )
    return activation, slope


def dot(a, b, precision=None):
    return jnp.dot(a, b, preferred_element_type=F32, precision=precision)


def dot_nt(a, b, precision=None):
    return lax.dot_general(
        a, b, (((1,), (1,)), ((), ())), preferred_element_type=F32, precision=precision
    )


def subsets(items):
    found = [()]
    for item in items:
        found += [s + (item,) for s in found]
    return found


def kernel(
    n, g, rank, n_recv,
    tok, cot, w_gate, w_up, w_down, err, q_pad,
    tok_grad, new_err, p_out, q_out,
    full, tok_t, cot_t, act, ups, hid, d_up, d_gate, grads, *rest
):
    recv_bufs = rest[:n_recv]
    (merged, power, hat, block_diag, q_t, pw_all, gram_all, q_part, q_rs, q_grp, q_all,
     send_sems, recv_sems, local_sems) = rest[n_recv:]
    me, grp = lax.axis_index("node"), lax.axis_index("grp")
    rows, hidden = w_gate.shape
    depth = tok.shape[1]
    half = hidden // 2
    bits = n.bit_length() - 1
    tile = 256
    used = 3 * rank
    weights = (w_gate, w_up, w_down)

    barrier = pltpu.get_barrier_semaphore()
    for d in range(1, n):
        pl.semaphore_signal(barrier, inc=1, device_id=(lax.rem(me + d, n), grp), device_id_type=MESH)
    for d in range(1, g):
        pl.semaphore_signal(barrier, inc=1, device_id=(me, lax.rem(grp + d, g)), device_id_type=MESH)

    flip = [(1 << b) * (1 - 2 * lax.rem(me // (1 << b), 2)) for b in range(bits)]
    offset = lambda mask: sum((flip[b] for b in mask), 0)
    outer = list(range(1, bits))
    orders = [outer + [0], outer[::-1] + [0]]
    rs_orders = [[0] + outer, [0] + outer[::-1]]
    cols = [pl.ds(h * half, half) for h in range(2)]
    block = lambda index: pl.ds(pl.multiple_of(index * rows, rows), rows)

    count = [0]
    started = []

    def send(src, dst, node, group):
        copy = pltpu.make_async_remote_copy(
            src_ref=src, dst_ref=dst,
            send_sem=send_sems.at[count[0]], recv_sem=recv_sems.at[count[0]],
            device_id=(node, group), device_id_type=MESH,
        )
        count[0] += 1
        started.append(copy)
        copy.start()
        return copy

    locals_ = []
    for w in range(3):
        copy = pltpu.make_async_copy(weights[w], full.at[w, block(me)], local_sems.at[w])
        copy.start()
        locals_.append(copy)
    pl.semaphore_wait(barrier, n - 1 + g - 1)

    gathers = {}

    def gather_send(w, t, h, mask):
        at = (w, block(me + offset(mask)), cols[h])
        src = full.at[at] if mask else weights[w].at[:, cols[h]]
        copy = send(src, full.at[at], me + flip[orders[h][t]], grp)
        gathers.setdefault((w, t, h), []).append(copy)

    def gather_start(w, t):
        for h in range(2):
            held = subsets(orders[h][:t])
            if t < bits - 1:
                for mask in held:
                    gather_send(w, t, h, mask)
            for mask in held:
                if t == 0 or orders[h][t - 1] in mask:
                    gather_send(w, bits - 1, h, mask)

    def gather_finish(w, t):
        for h in range(2):
            for copy in gathers[w, t, h]:
                copy.wait_recv()

    for w in range(2):
        gather_start(w, 0)

    @pl.loop(0, depth // tile)
    def _(i):
        at = pl.ds(pl.multiple_of(i * tile, tile), tile)
        tok_t[at, :] = tok[:, at].T
        cot_t[at, :] = cot[:, at].T

    merged[...] = jnp.zeros_like(merged)
    power[...] = jnp.zeros_like(power)
    hat[...] = jnp.zeros_like(hat)
    block_diag[...] = jnp.zeros_like(block_diag)
    q_t[...] = jnp.zeros_like(q_t)
    for copy in locals_:
        copy.wait()

    for t in range(1, bits - 1):
        for w in range(2):
            gather_finish(w, t - 1)
            gather_start(w, t)
    gather_start(2, 0)
    gather_finish(0, bits - 2)
    gather_start(0, bits - 1)
    gather_finish(0, bits - 1)

    @pl.loop(0, hidden // tile)
    def _(j):
        at = pl.ds(pl.multiple_of(j * tile, tile), tile)
        act[:, at] = dot(tok[...], full[0, :, at])

    gather_finish(1, bits - 2)
    gather_start(1, bits - 1)
    gather_finish(1, bits - 1)

    def up_part(first, last):
        @pl.loop(first, last)
        def _(j):
            at = pl.ds(pl.multiple_of(j * tile, tile), tile)
            up_pre = dot(tok[...], full[1, :, at])
            activation, slope = gelu_parts(act[:, at])
            act[:, at] = activation
            ups[:, at] = up_pre * slope
            hid[:, at] = (activation * up_pre).astype(BF16)

    tiles = hidden // tile
    up_part(0, tiles // 2)
    for t in range(1, bits - 1):
        gather_finish(2, t - 1)
        gather_start(2, t)
    up_part(tiles // 2, tiles)

    reduces = {}

    steps = depth // tile

    def partial_grad(m, left, right, first=0, last=steps):
        @pl.loop(first, last)
        def _(i):
            at = pl.ds(pl.multiple_of(i * tile, tile), tile)
            grads[m, at, :] = dot(left[at, :], right[...]).astype(BF16)

    def reduce_start(m, t):
        for h in range(2):
            bit = rs_orders[h][t]
            reduces[m, t, h] = []
            for slot, mask in enumerate(subsets(rs_orders[h][t + 1:])):
                src = grads.at[m, block(me + flip[bit] + offset(mask)), cols[h]]
                dst = recv_bufs[t].at[m, slot, :, cols[h]]
                reduces[m, t, h].append(send(src, dst, me + flip[bit], grp))

    def reduce_add(m, t):
        for h in range(2):
            for slot, mask in enumerate(subsets(rs_orders[h][t + 1:])):
                reduces[m, t, h][slot].wait_recv()
                at = block(me + offset(mask))
                total = (
                    grads[m, at, cols[h]].astype(F32) + recv_bufs[t][m, slot, :, cols[h]].astype(F32)
                )
                if t < bits - 1:
                    grads[m, at, cols[h]] = total.astype(BF16)
                else:
                    scale = 1.0 / math.sqrt(tok.shape[0] * n)
                    memory = err[0, :, pl.ds(m * hidden + h * half, half)].astype(F32)
                    merged[m, 0:rows, cols[h]] = total * scale + memory

    def advance(m, t):
        reduce_add(m, t - 1)
        reduce_start(m, t)

    partial_grad(2, cot_t, hid)
    reduce_start(2, 0)
    gather_finish(2, bits - 2)
    gather_start(2, bits - 1)
    advance(2, 1)
    gather_finish(2, bits - 1)

    @pl.loop(0, hidden // tile)
    def _(j):
        at = pl.ds(pl.multiple_of(j * tile, tile), tile)
        back = dot(cot[...], full[2, :, at])
        d_up[:, at] = (back * act[:, at]).astype(BF16)
        d_gate[:, at] = (back * ups[:, at]).astype(BF16)

    partial_grad(0, tok_t, d_gate)
    reduce_start(0, 0)
    advance(2, 2)
    partial_grad(1, tok_t, d_up, 0, steps // 2)
    advance(0, 1)
    partial_grad(1, tok_t, d_up, steps // 2, steps)
    reduce_start(1, 0)

    def token_part(first, last):
        @pl.loop(first, last)
        def _(i):
            at = pl.ds(pl.multiple_of(i * tile, tile), tile)
            tok_grad[:, at] = (
                dot_nt(d_gate[...], full[0, at, :]) + dot_nt(d_up[...], full[1, at, :])
            ).astype(BF16)

    token_part(0, steps // 3)
    advance(1, 1)
    token_part(steps // 3, 2 * steps // 3)
    advance(0, 2)
    token_part(2 * steps // 3, steps)
    advance(1, 2)
    for t in range(3, bits):
        for m in (2, 0, 1):
            advance(m, t)
    total = jnp.zeros((rows, LANES), F32)
    for m in (2, 0, 1):
        reduce_add(m, bits - 1)
        total += dot(merged[m, 0:rows, :], q_pad[m], HIGHEST)

    pw_all[grp] = total.astype(BF16)
    copies = [
        send(pw_all.at[grp], pw_all.at[grp], me, lax.rem(grp + d, g)) for d in range(1, g)
    ]
    for copy in copies:
        copy.wait_recv()
    total = pw_all[0].astype(F32)
    for k in range(1, g):
        total += pw_all[k].astype(F32)
    power[0:rows, :] = total * (1.0 / g)

    lane = lax.broadcasted_iota(jnp.int32, (rank, LANES), 1)
    row = lax.broadcasted_iota(jnp.int32, (rank, LANES), 0)
    padded = power[...]
    gram = dot(padded.T, padded, HIGHEST)
    picked = gram[0:rank]
    for m in range(1, 3):
        picked = jnp.where(lane >= m * rank, gram[m * rank:(m + 1) * rank], picked)
    gram_all[me] = picked
    copies = [
        send(gram_all.at[me], gram_all.at[me], lax.rem(me + d, n), grp) for d in range(1, n)
    ]
    for copy in copies:
        copy.wait_recv()
    picked = gram_all[0]
    for k in range(1, n):
        picked += gram_all[k]

    work = []
    for m in range(3):
        rolled = picked if m == 0 else pltpu.roll(picked, LANES - m * rank, 1)
        unit = jnp.where(lane == row + rank, 1.0, 0.0).astype(F32)
        work.append(jnp.where(lane < rank, rolled, unit))
    for j in range(rank):
        for m in range(3):
            a = work[m]
            inverse = 1.0 / jnp.sqrt(a[j:j + 1, j:j + 1])
            pivot_row = a[j:j + 1, :] * inverse
            column = a[:, j:j + 1] * inverse
            work[m] = jnp.where(row > j, a - column * pivot_row, jnp.where(row == j, pivot_row, a))
    for m in range(3):
        shift = ((m - 1) * rank) % LANES
        moved = work[m] if shift == 0 else pltpu.roll(work[m], shift, 1)
        inside = (lane >= m * rank) & (lane < (m + 1) * rank)
        block_diag[m * rank:(m + 1) * rank, :] = jnp.where(inside, moved, 0.0)
    hat[0:rows, :] = dot_nt(power[0:rows, :], block_diag[...], HIGHEST)
    p_out[...] = hat[0:rows, :]

    hat_t = hat[...].T
    c_blocks = min(n, hidden // LANES)
    r_blocks = n // c_blocks
    c_size, r_size = hidden // c_blocks, used // r_blocks
    for m in range(3):
        q_t[m * rank:(m + 1) * rank, :] = dot(hat_t[m * rank:(m + 1) * rank], merged[m], HIGHEST)
    spots = [
        (slice(c // c_blocks * r_size, (c // c_blocks + 1) * r_size),
         slice(c % c_blocks * c_size, (c % c_blocks + 1) * c_size))
        for c in range(n)
    ]
    for c in range(n):
        q_part[c] = q_t[spots[c]].astype(BF16)
    q_rs[me] = q_part[me]
    copies = []
    for d in range(1, n):
        to = lax.rem(me + d, n)
        copies.append(send(q_part.at[to], q_rs.at[me], to, grp))
    for copy in copies:
        copy.wait_recv()
    total = q_rs[0].astype(F32)
    for k in range(1, n):
        total += q_rs[k].astype(F32)
    q_grp[grp] = total.astype(BF16)
    copies = [send(q_grp.at[grp], q_grp.at[grp], me, lax.rem(grp + d, g)) for d in range(1, g)]
    for copy in copies:
        copy.wait_recv()
    total = q_grp[0].astype(F32)
    for k in range(1, g):
        total += q_grp[k].astype(F32)
    q_all[me] = (total * (1.0 / g)).astype(BF16)
    copies = [send(q_all.at[me], q_all.at[me], lax.rem(me + d, n), grp) for d in range(1, n)]
    for copy in copies:
        copy.wait_recv()
    for c in range(n):
        q_t[spots[c]] = q_all[c].astype(F32)
    q_out[...] = q_t[0:used, :]

    wide = lax.broadcasted_iota(jnp.int32, (rows, LANES), 1)
    for m in range(3):
        own = jnp.where((wide >= m * rank) & (wide < (m + 1) * rank), hat[0:rows, :], 0.0)
        for h in range(2):
            rebuilt = dot(own, q_t[:, cols[h]], HIGHEST)
            new_err[0, :, pl.ds(m * hidden + h * half, half)] = (
                merged[m, 0:rows, cols[h]] - rebuilt
            ).astype(BF16)
    for copy in started:
        copy.wait_send()


def on_device(n, g, tokens, cotangent, gate_weight, up_weight, down_weight_t, error_memory, q_init):
    token_rows, depth = tokens.shape
    rows, hidden = gate_weight.shape
    rank = q_init.shape[2]
    used = 3 * rank
    bits = n.bit_length() - 1
    padded = -(-rows // LANES) * LANES
    q_pad = jnp.stack(
        [jnp.pad(q_init[m], ((0, 0), (m * rank, LANES - (m + 1) * rank))) for m in range(3)]
    )
    c_blocks = min(n, hidden // LANES)
    chunk = (used // (n // c_blocks), hidden // c_blocks)
    copies = 12 * (n - 1) + 3 * (n - 1) + 2 * (g - 1)
    recv_shapes = [
        pltpu.VMEM((3, 1 << (bits - 1 - t), rows, hidden), BF16) for t in range(bits)
    ]
    vmem = pl.BlockSpec(memory_space=pltpu.VMEM)
    token_grad, new_error, hats, q_t = pl.pallas_call(
        functools.partial(kernel, n, g, rank, bits),
        out_shape=(
            jax.ShapeDtypeStruct((token_rows, depth), BF16),
            jax.ShapeDtypeStruct((1, rows, 3 * hidden), BF16),
            jax.ShapeDtypeStruct((rows, LANES), F32),
            jax.ShapeDtypeStruct((used, hidden), F32),
        ),
        in_specs=[vmem] * 7,
        out_specs=(vmem,) * 4,
        scratch_shapes=[
            pltpu.VMEM((3, depth, hidden), BF16),
            pltpu.VMEM((depth, token_rows), BF16),
            pltpu.VMEM((depth, token_rows), BF16),
            pltpu.VMEM((token_rows, hidden), F32),
            pltpu.VMEM((token_rows, hidden), F32),
            pltpu.VMEM((token_rows, hidden), BF16),
            pltpu.VMEM((token_rows, hidden), BF16),
            pltpu.VMEM((token_rows, hidden), BF16),
            pltpu.VMEM((3, depth, hidden), BF16),
            *recv_shapes,
            pltpu.VMEM((3, padded, hidden), F32),
            pltpu.VMEM((padded, LANES), F32),
            pltpu.VMEM((padded, LANES), F32),
            pltpu.VMEM((LANES, LANES), F32),
            pltpu.VMEM((LANES, hidden), F32),
            pltpu.VMEM((g, rows, LANES), BF16),
            pltpu.VMEM((n, rank, LANES), F32),
            pltpu.VMEM((n,) + chunk, BF16),
            pltpu.VMEM((n,) + chunk, BF16),
            pltpu.VMEM((g,) + chunk, BF16),
            pltpu.VMEM((n,) + chunk, BF16),
            pltpu.SemaphoreType.DMA((copies,)),
            pltpu.SemaphoreType.DMA((copies,)),
            pltpu.SemaphoreType.DMA((3,)),
        ],
        compiler_params=pltpu.CompilerParams(
            collective_id=0, has_side_effects=True, vmem_limit_bytes=67_043_328
        ),
    )(tokens, cotangent, gate_weight, up_weight, down_weight_t, error_memory, q_pad)
    p_hat = jnp.stack([hats[:, m * rank:(m + 1) * rank] for m in range(3)])
    q_new = q_t.reshape(3, rank, hidden).transpose(0, 2, 1)
    return token_grad, new_error, p_hat, q_new


def solution(mesh):
    return jax.shard_map(
        functools.partial(on_device, mesh.shape["node"], mesh.shape["grp"]),
        mesh=mesh,
        in_specs=(
            P(("node", "grp"), None),
            P(("node", "grp"), None),
            P("node", None),
            P("node", None),
            P("node", None),
            P("grp", "node", None),
            P(),
        ),
        out_specs=(P(("node", "grp"), None), P("grp", "node", None), P(None, "node", None), P()),
        check_vma=False,
    )
```
